32 devices in a mesh: mem: 4 (over y, x), cell: 8 (over z, core).
Axes of the slice: x: 2, y: 2, z: 4, core: 2. Of those that a mesh axis runs over, the one named last changes fastest.
Arguments:
- state: bfloat16 [16384, 40, 120], P('cell', 'mem'), may hold values from -6 to 6
- vertical_weight: bfloat16 [8192, 120], P('cell'), may hold values from -0.5 to 0.5
- horizontal_weight: float32 [8192, 4], P('cell'), may hold values from 0.05 to 0.45
- obs_slot: int32 [8192, 4], P('cell'), may hold values from 0 to 4095, as said below
- request_cell: int32 [8, 4096], P('cell'), may hold values from 0 to 2047
- obs_value: float32 [8192], P('cell'), may hold values from -6 to 6
- obs_error: float32 [8192], P('cell'), may hold values from 0.5 to 2
- obs_region: int32 [8192], P('cell'), may hold values from 0 to 63, as said below
Outputs:
- cov_matrix: float32 [64, 40, 40], P('cell', 'mem')
- innovation_proj: float32 [64, 40], P('cell', 'mem')
The draws below stay inside these ranges and needn't reach their ends.
Inputs may be any that keep to these rules, and one draw needn't show every extreme that they name: `obs_slot`: within one owner's 1024 observations all 4096 slots differ, so every slot is used: 1024 ask the owner's own patch and 768 each of the four patches at distance 1 and 2. `obs_region`: an observation's region is one of the 8 regions of its owner's patch or of the patches just before or after it (indices wrap); patch p holds regions p * 8 to p * 8 + 7.
All inputs are finite; a program needn't handle non-finite values.
Results may differ from the reference program's by a relative error of at most 0.0003.
Values may be sent and summed in bfloat16 or wider, within the bound.
A program may use at most 128 MiB of HBM per device.

```python
import math
import jax
import jax.numpy as jnp
from jax import lax

MEMBERS = 40
LEV = 120
NEIGH = 4
CELL_DEV = 2048
OBS_DEV = 1024
REG_DEV = 8
HALO_CAP = 768
OWN_CAP = 1024
CELLS = 16384
OBS = 8192
REGIONS = 64
N_CELL = 8


def routing(key):
    base = jax.random.fold_in(key, 71)

    def one_owner(owner_key):
        key_perm, key_cell = jax.random.split(owner_key, 2)
        total = 4 * OBS_DEV
        chosen = jax.random.permutation(key_perm, total).astype(jnp.int32).reshape(OBS_DEV, NEIGH)
        cells = jax.random.randint(key_cell, (total,), 0, CELL_DEV).astype(jnp.int32)
        return (chosen, cells)
    keys = jax.random.split(base, N_CELL)
    chosen, cells = jax.vmap(one_owner)(keys)
    return (chosen.reshape(OBS, NEIGH), cells.reshape(N_CELL, 4 * OBS_DEV))


def draw_obs_slot(key, part):
    return routing(key)[0]


def draw_request_cell(key, part):
    return routing(key)[1]


def draw_obs_region(key, part):
    key_side, key_within = jax.random.split(jax.random.fold_in(key, 53), 2)
    code = jax.random.randint(key_side, (N_CELL, OBS_DEV), 0, 4).astype(jnp.int32)
    moves = jnp.array([-1, 0, 0, 1], dtype=jnp.int32)[code]
    owner = jnp.arange(N_CELL, dtype=jnp.int32)[:, None]
    patch = jnp.mod(owner + moves, N_CELL).astype(jnp.int32)
    within = jax.random.randint(key_within, (N_CELL, OBS_DEV), 0, REG_DEV).astype(jnp.int32)
    return (patch * REG_DEV + within).reshape(OBS).astype(jnp.int32)


def block_scale(rng, shape, shards, least, top_value):
    def one(position, parts):
        heights = jax.random.uniform(jax.random.fold_in(jax.random.fold_in(rng, 6), position), (parts,), jnp.float32, least / len(shards), top_value / len(shards))
        return jnp.repeat(jnp.exp(heights), shape[position] // parts).reshape((-1,) + (1,) * (len(shape) - position - 1))

    factor_of = one(*shards[0])
    for cut in shards[1:]:
        factor_of = factor_of * one(*cut)
    return factor_of


def bell_draw(rng, shape, scale, most, shards=(), held_as=jnp.bfloat16):
    loudness = block_scale(rng, shape, shards, -0.22, 0.18) if shards else 1.0
    values = jax.random.normal(rng, shape, jnp.float32) * scale * loudness
    return jnp.minimum(jnp.maximum(values, -most), most).astype(held_as)


def setup_inputs(seed: int = 0) -> dict:
    key_list = jax.random.split(jax.random.key(seed), 9)
    return {
        "state": bell_draw(key_list[0], (CELLS, MEMBERS, LEV), 1.0, 6.0, ((0, 8), (1, 4))),
        "vertical_weight": bell_draw(key_list[1], (OBS, LEV), LEV ** -0.5, 0.5, ((0, 8),)),
        "horizontal_weight": jnp.clip(0.05 + 0.39999999 * jax.random.uniform(key_list[2], (OBS, NEIGH), jnp.float32) ** block_scale(key_list[2], (OBS, NEIGH), ((0, 8),), -0.2, 0.2), 0.05, 0.45),
        "obs_slot": draw_obs_slot(jax.random.fold_in(key_list[8], 71), 0),
        "request_cell": draw_request_cell(jax.random.fold_in(key_list[8], 71), 0),
        "obs_value": bell_draw(key_list[5], (OBS,), 1.0, 6.0, ((0, 8),), jnp.float32),
        "obs_error": jnp.clip(jnp.exp(math.log(2.0) - 1.3862944 * jax.random.uniform(key_list[6], (OBS,), jnp.float32) ** block_scale(key_list[6], (OBS,), ((0, 8),), -0.2, 0.2)), 0.5, 2.0),
        "obs_region": draw_obs_region(jax.random.fold_in(key_list[8], 71), 0),
    }


def reference(state, vertical_weight, horizontal_weight, obs_slot, request_cell, obs_value, obs_error, obs_region):
    halo_moves = jnp.array([-2, -1, 1, 2], dtype=jnp.int32)

    def block(src):
        slots = lax.dynamic_slice_in_dim(obs_slot, src * OBS_DEV, OBS_DEV, 0)
        table = lax.dynamic_slice_in_dim(request_cell, src, 1, 0)[0]
        within = table[slots]
        which = jnp.minimum(jnp.maximum(slots - OWN_CAP, 0) // HALO_CAP, 3).astype(jnp.int32)
        moved = jnp.mod(src + halo_moves[which], N_CELL).astype(jnp.int32)
        patch = jnp.where(slots < OWN_CAP, src, moved).astype(jnp.int32)
        cells = (patch * CELL_DEV + within).astype(jnp.int32)
        picked = state[cells].astype(jnp.float32)
        levels = lax.dynamic_slice_in_dim(vertical_weight, src * OBS_DEV, OBS_DEV, 0).astype(jnp.float32)
        column = jnp.einsum('okml,ol->okm', picked, levels)
        horiz = lax.dynamic_slice_in_dim(horizontal_weight, src * OBS_DEV, OBS_DEV, 0)
        return jnp.sum(column * horiz[:, :, None], axis=1)

    equiv = lax.map(block, jnp.arange(N_CELL, dtype=jnp.int32)).reshape(OBS, MEMBERS)
    mean = jnp.mean(equiv, axis=1, keepdims=True)
    spread = equiv - mean
    inverse = 1.0 / (obs_error * obs_error)
    innov = (obs_value - mean[:, 0]) * inverse

    def accumulate(carry, src):
        part = lax.dynamic_slice_in_dim(spread, src * OBS_DEV, OBS_DEV, 0)
        scale = lax.dynamic_slice_in_dim(inverse, src * OBS_DEV, OBS_DEV, 0)
        drive = lax.dynamic_slice_in_dim(innov, src * OBS_DEV, OBS_DEV, 0)
        region = lax.dynamic_slice_in_dim(obs_region, src * OBS_DEV, OBS_DEV, 0)
        outer = part[:, :, None] * part[:, None, :] * scale[:, None, None]
        vector = part * drive[:, None]
        total_cov = carry[0] + jax.ops.segment_sum(outer, region, num_segments=REGIONS)
        total_vec = carry[1] + jax.ops.segment_sum(vector, region, num_segments=REGIONS)
        return (total_cov, total_vec), None

    start = (jnp.zeros((REGIONS, MEMBERS, MEMBERS), jnp.float32), jnp.zeros((REGIONS, MEMBERS), jnp.float32))
    result, unused = lax.scan(accumulate, start, jnp.arange(N_CELL, dtype=jnp.int32))
    return result[0], result[1]
```

```python
import functools

import jax
import jax.numpy as jnp
from jax import lax
from jax.experimental import pallas as pl
from jax.experimental.pallas import tpu as pltpu
from jax.sharding import PartitionSpec as P

REG_DEV = 8
GROUP = 128


halo_moves = (-2, -1, 1, 2)


def passed_along(x, axis, by):
    devices = lax.axis_size(axis)
    return lax.ppermute(x, axis, [(i, (i + by) % devices) for i in range(devices)])


def bf16_parts(x, count):
    parts = []
    rest = x
    for _ in range(count):
        top = lax.reduce_precision(rest, 8, 7)
        parts.append(top.astype(jnp.bfloat16))
        rest = rest - top
    return parts


def column_kernel(requests, cell_ref, row_ref, state_ref, weight_ref, out_ref, wide_ref):
    wide_ref[...] = weight_ref[...].astype(jnp.float32)
    members = state_ref.shape[1]
    lane = lax.broadcasted_iota(jnp.int32, (members, GROUP), 1)

    def group(g, carry):
        first = pl.multiple_of(g * GROUP, GROUP)
        total = jnp.zeros((members, GROUP), jnp.float32)
        for j in range(GROUP):
            column = state_ref[cell_ref[first + j]].astype(jnp.float32)
            weights = wide_ref[pl.ds(row_ref[first + j], 1), :]
            dot = jnp.sum(column * weights, axis=1, keepdims=True)
            total = jnp.where(lane == j, dot, total)
        out_ref[:, pl.ds(first, GROUP)] = total
        return carry

    lax.fori_loop(0, requests // GROUP, group, 0)


def columns(cell, row, state, weight):
    requests = cell.shape[0]
    cells, members, levels = state.shape
    return pl.pallas_call(
        functools.partial(column_kernel, requests),
        out_shape=jax.ShapeDtypeStruct((members, requests), jnp.float32),
        in_specs=[
            pl.BlockSpec(memory_space=pltpu.SMEM),
            pl.BlockSpec(memory_space=pltpu.SMEM),
            pl.BlockSpec(memory_space=pltpu.VMEM),
            pl.BlockSpec(memory_space=pltpu.VMEM),
        ],
        out_specs=pl.BlockSpec(memory_space=pltpu.VMEM),
        scratch_shapes=[pltpu.VMEM(weight.shape, jnp.float32)],
        compiler_params=pltpu.CompilerParams(vmem_limit_bytes=40 * 2**20),
        cost_estimate=pl.CostEstimate(
            flops=2 * requests * members * levels, bytes_accessed=2 * state.size, transcendentals=0
        ),
    )(cell, row, state, weight)


def on_device(
    state,
    vertical_weight,
    horizontal_weight,
    obs_slot,
    request_cell,
    obs_value,
    obs_error,
    obs_region,
):
    patches = lax.axis_size("cell")
    here = lax.axis_index("cell")
    cell_dev, mem_dev, levels = state.shape
    obs_dev, neigh = obs_slot.shape
    halo_cap = 3 * obs_dev // 4
    total_slots = 4 * obs_dev
    table = request_cell.reshape(-1)
    arrived = [passed_along(vertical_weight, "cell", offset) for offset in halo_moves]

    lanes = 128
    rows = total_slots // lanes
    slots = obs_slot.T.reshape(-1)
    hweights = horizontal_weight.T.reshape(-1)
    obs_of = lax.iota(jnp.int32, total_slots) % obs_dev
    terms = [(obs_of // 32).astype(jnp.bfloat16), (obs_of % 32).astype(jnp.bfloat16)]
    terms += bf16_parts(hweights, 3)
    high = lax.iota(jnp.int32, rows)[:, None] == (slots // lanes)[None, :]
    low = lax.iota(jnp.int32, lanes)[:, None] == (slots % lanes)[None, :]
    left = jnp.concatenate(
        [jnp.where(high, term[None, :], jnp.bfloat16(0)) for term in terms], axis=0
    )
    by_slot = lax.dot_general(
        left,
        low.astype(jnp.bfloat16),
        (((1,), (1,)), ((), ())),
        preferred_element_type=jnp.float32,
    ).reshape(len(terms), total_slots)
    slot_obs = (by_slot[0] * 32 + by_slot[1] + 0.5).astype(jnp.int32)
    slot_hweight = by_slot[2] + by_slot[3] + by_slot[4]

    asked = jnp.stack([table, slot_obs])
    cells_asked = [table[:obs_dev]]
    rows_asked = [slot_obs[:obs_dev]]
    for number, offset in enumerate(halo_moves):
        lower = obs_dev + number * halo_cap
        wanted = passed_along(asked[:, lower : lower + halo_cap], "cell", offset)
        cells_asked.append(wanted[0])
        rows_asked.append(wanted[1] + (number + 1) * obs_dev)
    found = columns(
        jnp.concatenate(cells_asked),
        jnp.concatenate(rows_asked),
        state,
        jnp.concatenate([vertical_weight] + arrived, axis=0),
    )
    pieces = [found[:, :obs_dev]]
    for number, offset in enumerate(halo_moves):
        lower = obs_dev + number * halo_cap
        pieces.append(passed_along(found[:, lower : lower + halo_cap], "cell", -offset))
    equiv = jnp.concatenate(pieces, axis=1) * slot_hweight[None, :]
    mixing = (slot_obs[:, None] == lax.iota(jnp.int32, obs_dev)[None, :]).astype(jnp.bfloat16)
    own_parts = jnp.dot(
        jnp.concatenate(bf16_parts(equiv, 3), axis=0),
        mixing,
        preferred_element_type=jnp.float32,
    )
    own_equiv = own_parts.reshape(3, mem_dev, obs_dev).sum(axis=0)
    everyone = lax.all_gather(own_equiv, "mem", axis=0, tiled=True)
    mean = jnp.mean(everyone, axis=0, keepdims=True)
    spread_all = everyone - mean
    spread_own = own_equiv - mean
    members = everyone.shape[0]
    inverse = 1.0 / (obs_error * obs_error)
    innov = (obs_value - mean[0]) * inverse
    reg_dev = REG_DEV
    relative = jnp.mod(obs_region - (here - 1) * reg_dev, patches * reg_dev)
    region_ids = lax.iota(jnp.int32, 3 * reg_dev)
    onehot = (region_ids[:, None] == relative[None, :]).astype(jnp.float32)
    masked = (onehot[:, None, :] * spread_own[None, :, :]).reshape(3 * reg_dev * mem_dev, obs_dev)
    scaled_all = spread_all * inverse[None, :]
    cov_part = lax.dot_general(
        masked,
        scaled_all,
        (((1,), (1,)), ((), ())),
        precision=lax.Precision.HIGHEST,
        preferred_element_type=jnp.float32,
    )
    vec_part = jnp.dot(
        masked, innov, precision=lax.Precision.HIGHEST, preferred_element_type=jnp.float32
    )
    sums = jnp.concatenate(
        [cov_part.reshape(3 * reg_dev, mem_dev * members), vec_part.reshape(3 * reg_dev, mem_dev)],
        axis=1,
    )
    from_prev = passed_along(sums[2 * reg_dev :], "cell", 1)
    from_next = passed_along(sums[:reg_dev], "cell", -1)
    summed = sums[reg_dev : 2 * reg_dev] + from_prev + from_next
    cov_matrix = summed[:, : mem_dev * members].reshape(reg_dev, mem_dev, members)
    innovation_proj = summed[:, mem_dev * members :]
    return (cov_matrix, innovation_proj)


def solution(mesh):
    in_specs = (
        P("cell", "mem", None),
        P("cell", None),
        P("cell", None),
        P("cell", None),
        P("cell", None),
        P("cell"),
        P("cell"),
        P("cell"),
    )
    out_specs = (P("cell", "mem", None), P("cell", "mem"))
    return jax.shard_map(
        on_device, mesh=mesh, in_specs=in_specs, out_specs=out_specs, check_vma=False
    )
```

```python
import functools

import jax
import jax.numpy as jnp
from jax import lax
from jax.experimental import pallas as pl
from jax.experimental.pallas import tpu as pltpu
from jax.sharding import PartitionSpec as P

REG_DEV = 8
GROUP = 128


halo_moves = (-2, -1, 1, 2)


def passed_along(x, axis, by):
    devices = lax.axis_size(axis)
    return lax.ppermute(x, axis, [(i, (i + by) % devices) for i in range(devices)])


def bf16_parts(x, count):
    parts = []
    rest = x
    for _ in range(count):
        top = lax.reduce_precision(rest, 8, 7)
        parts.append(top.astype(jnp.bfloat16))
        rest = rest - top
    return parts


def column_kernel(requests, cell_ref, row_ref, state_ref, weight_ref, out_ref, wide_ref):
    wide_ref[...] = weight_ref[...].astype(jnp.float32)
    members = state_ref.shape[1]
    lane = lax.broadcasted_iota(jnp.int32, (members, GROUP), 1)

    def group(g, carry):
        first = pl.multiple_of(g * GROUP, GROUP)
        total = jnp.zeros((members, GROUP), jnp.float32)
        for j in range(GROUP):
            column = state_ref[cell_ref[first + j]].astype(jnp.float32)
            weights = wide_ref[pl.ds(row_ref[first + j], 1), :]
            dot = jnp.sum(column * weights, axis=1, keepdims=True)
            total = jnp.where(lane == j, dot, total)
        out_ref[:, pl.ds(first, GROUP)] = total
        return carry

    lax.fori_loop(0, requests // GROUP, group, 0)


def columns(cell, row, state, weight):
    requests = cell.shape[0]
    cells, members, levels = state.shape
    return pl.pallas_call(
        functools.partial(column_kernel, requests),
        out_shape=jax.ShapeDtypeStruct((members, requests), jnp.float32),
        in_specs=[
            pl.BlockSpec(memory_space=pltpu.SMEM),
            pl.BlockSpec(memory_space=pltpu.SMEM),
            pl.BlockSpec(memory_space=pltpu.VMEM),
            pl.BlockSpec(memory_space=pltpu.VMEM),
        ],
        out_specs=pl.BlockSpec(memory_space=pltpu.VMEM),
        scratch_shapes=[pltpu.VMEM(weight.shape, jnp.float32)],
        compiler_params=pltpu.CompilerParams(vmem_limit_bytes=40 * 2**20),
        cost_estimate=pl.CostEstimate(
            flops=2 * requests * members * levels, bytes_accessed=2 * state.size, transcendentals=0
        ),
    )(cell, row, state, weight)


def on_device(
    state,
    vertical_weight,
    horizontal_weight,
    obs_slot,
    request_cell,
    obs_value,
    obs_error,
    obs_region,
):
    patches = lax.axis_size("cell")
    here = lax.axis_index("cell")
    cell_dev, mem_dev, levels = state.shape
    obs_dev, neigh = obs_slot.shape
    halo_cap = 3 * obs_dev // 4
    total_slots = 4 * obs_dev
    table = request_cell.reshape(-1)
    sharers = lax.axis_size("mem")
    member = lax.axis_index("mem")
    part_dev = obs_dev // sharers
    part = lax.dynamic_slice_in_dim(vertical_weight, member * part_dev, part_dev, 0)
    mine = jnp.concatenate([passed_along(part, "cell", offset) for offset in halo_moves], axis=0)
    weight = jnp.concatenate(
        [mine] + [passed_along(mine, "mem", by) for by in range(1, sharers)] + [vertical_weight],
        axis=0,
    )

    lanes = 128
    rows = total_slots // lanes
    slots = obs_slot.T.reshape(-1)
    hweights = horizontal_weight.T.reshape(-1)
    obs_of = lax.iota(jnp.int32, total_slots) % obs_dev
    terms = [(obs_of // 32).astype(jnp.bfloat16), (obs_of % 32).astype(jnp.bfloat16)]
    terms += bf16_parts(hweights, 3)
    high = lax.iota(jnp.int32, rows)[:, None] == (slots // lanes)[None, :]
    low = lax.iota(jnp.int32, lanes)[:, None] == (slots % lanes)[None, :]
    left = jnp.concatenate(
        [jnp.where(high, term[None, :], jnp.bfloat16(0)) for term in terms], axis=0
    )
    by_slot = lax.dot_general(
        left,
        low.astype(jnp.bfloat16),
        (((1,), (1,)), ((), ())),
        preferred_element_type=jnp.float32,
    ).reshape(len(terms), total_slots)
    slot_obs = (by_slot[0] * 32 + by_slot[1] + 0.5).astype(jnp.int32)
    slot_hweight = by_slot[2] + by_slot[3] + by_slot[4]

    asked = jnp.stack([table, slot_obs])
    cells_asked = [table[:obs_dev]]
    rows_asked = [slot_obs[:obs_dev] + len(halo_moves) * obs_dev]
    for number, offset in enumerate(halo_moves):
        lower = obs_dev + number * halo_cap
        wanted = passed_along(asked[:, lower : lower + halo_cap], "cell", offset)
        cells_asked.append(wanted[0])
        shift = jnp.mod(member - wanted[1] // part_dev, sharers)
        rows_asked.append(
            (shift * len(halo_moves) + number) * part_dev + jnp.mod(wanted[1], part_dev)
        )
    found = columns(
        jnp.concatenate(cells_asked),
        jnp.concatenate(rows_asked),
        state,
        weight,
    )
    pieces = [found[:, :obs_dev]]
    for number, offset in enumerate(halo_moves):
        lower = obs_dev + number * halo_cap
        pieces.append(passed_along(found[:, lower : lower + halo_cap], "cell", -offset))
    equiv = jnp.concatenate(pieces, axis=1) * slot_hweight[None, :]
    mixing = (slot_obs[:, None] == lax.iota(jnp.int32, obs_dev)[None, :]).astype(jnp.bfloat16)
    own_parts = jnp.dot(
        jnp.concatenate(bf16_parts(equiv, 3), axis=0),
        mixing,
        preferred_element_type=jnp.float32,
    )
    own_equiv = own_parts.reshape(3, mem_dev, obs_dev).sum(axis=0)
    everyone = jnp.zeros((sharers, mem_dev, obs_dev), jnp.float32)
    everyone = lax.dynamic_update_index_in_dim(everyone, own_equiv, member, 0)
    for by in range(1, sharers):
        everyone = lax.dynamic_update_index_in_dim(
            everyone, passed_along(own_equiv, "mem", by), jnp.mod(member - by, sharers), 0
        )
    everyone = everyone.reshape(sharers * mem_dev, obs_dev)
    mean = jnp.mean(everyone, axis=0, keepdims=True)
    spread_all = everyone - mean
    spread_own = own_equiv - mean
    members = everyone.shape[0]
    inverse = 1.0 / (obs_error * obs_error)
    innov = (obs_value - mean[0]) * inverse
    reg_dev = REG_DEV
    relative = jnp.mod(obs_region - (here - 1) * reg_dev, patches * reg_dev)
    region_ids = lax.iota(jnp.int32, 3 * reg_dev)
    onehot = (region_ids[:, None] == relative[None, :]).astype(jnp.float32)
    masked = (onehot[:, None, :] * spread_own[None, :, :]).reshape(3 * reg_dev * mem_dev, obs_dev)
    scaled_all = spread_all * inverse[None, :]
    cov_part = lax.dot_general(
        masked,
        scaled_all,
        (((1,), (1,)), ((), ())),
        precision=lax.Precision.HIGHEST,
        preferred_element_type=jnp.float32,
    )
    vec_part = jnp.dot(
        masked, innov, precision=lax.Precision.HIGHEST, preferred_element_type=jnp.float32
    )
    sums = jnp.concatenate(
        [cov_part.reshape(3 * reg_dev, mem_dev * members), vec_part.reshape(3 * reg_dev, mem_dev)],
        axis=1,
    )
    from_prev = passed_along(sums[2 * reg_dev :], "cell", 1)
    from_next = passed_along(sums[:reg_dev], "cell", -1)
    summed = sums[reg_dev : 2 * reg_dev] + from_prev + from_next
    cov_matrix = summed[:, : mem_dev * members].reshape(reg_dev, mem_dev, members)
    innovation_proj = summed[:, mem_dev * members :]
    return (cov_matrix, innovation_proj)


def solution(mesh):
    in_specs = (
        P("cell", "mem", None),
        P("cell", None),
        P("cell", None),
        P("cell", None),
        P("cell", None),
        P("cell"),
        P("cell"),
        P("cell"),
    )
    out_specs = (P("cell", "mem", None), P("cell", "mem"))
    return jax.shard_map(
        on_device, mesh=mesh, in_specs=in_specs, out_specs=out_specs, check_vma=False
    )
```

```python
import functools

import jax
import jax.numpy as jnp
from jax import lax
from jax.experimental import pallas as pl
from jax.experimental.pallas import tpu as pltpu
from jax.sharding import PartitionSpec as P

REG_DEV = 8
GROUP = 128


halo_moves = (-2, -1, 1, 2)


def passed_along(x, axis, by):
    devices = lax.axis_size(axis)
    return lax.ppermute(x, axis, [(i, (i + by) % devices) for i in range(devices)])


def bf16_parts(x, count):
    parts = []
    rest = x
    for _ in range(count):
        top = lax.reduce_precision(rest, 8, 7)
        parts.append(top.astype(jnp.bfloat16))
        rest = rest - top
    return parts


def column_kernel(requests, cell_ref, row_ref, state_ref, weight_ref, out_ref, wide_ref):
    wide_ref[...] = weight_ref[...].astype(jnp.float32)
    members = state_ref.shape[1]
    lane = lax.broadcasted_iota(jnp.int32, (members, GROUP), 1)

    def group(g, carry):
        first = pl.multiple_of(g * GROUP, GROUP)
        total = jnp.zeros((members, GROUP), jnp.float32)
        for j in range(GROUP):
            column = state_ref[cell_ref[first + j]].astype(jnp.float32)
            weights = wide_ref[pl.ds(row_ref[first + j], 1), :]
            dot = jnp.sum(column * weights, axis=1, keepdims=True)
            total = jnp.where(lane == j, dot, total)
        out_ref[:, pl.ds(first, GROUP)] = total
        return carry

    lax.fori_loop(0, requests // GROUP, group, 0)


def columns(cell, row, state, weight):
    requests = cell.shape[0]
    cells, members, levels = state.shape
    return pl.pallas_call(
        functools.partial(column_kernel, requests),
        out_shape=jax.ShapeDtypeStruct((members, requests), jnp.float32),
        in_specs=[
            pl.BlockSpec(memory_space=pltpu.SMEM),
            pl.BlockSpec(memory_space=pltpu.SMEM),
            pl.BlockSpec(memory_space=pltpu.VMEM),
            pl.BlockSpec(memory_space=pltpu.VMEM),
        ],
        out_specs=pl.BlockSpec(memory_space=pltpu.VMEM),
        scratch_shapes=[pltpu.VMEM(weight.shape, jnp.float32)],
        compiler_params=pltpu.CompilerParams(vmem_limit_bytes=40 * 2**20),
        cost_estimate=pl.CostEstimate(
            flops=2 * requests * members * levels, bytes_accessed=2 * state.size, transcendentals=0
        ),
    )(cell, row, state, weight)


def on_device(
    state,
    vertical_weight,
    horizontal_weight,
    obs_slot,
    request_cell,
    obs_value,
    obs_error,
    obs_region,
):
    patches = lax.axis_size("cell")
    here = lax.axis_index("cell")
    cell_dev, mem_dev, levels = state.shape
    obs_dev, neigh = obs_slot.shape
    halo_cap = 3 * obs_dev // 4
    total_slots = 4 * obs_dev
    table = request_cell.reshape(-1)
    arrived = [passed_along(vertical_weight, "cell", offset) for offset in halo_moves]

    lanes = 128
    rows = total_slots // lanes
    slots = obs_slot.T.reshape(-1)
    hweights = horizontal_weight.T.reshape(-1)
    obs_of = lax.iota(jnp.int32, total_slots) % obs_dev
    terms = [(obs_of // 32).astype(jnp.bfloat16), (obs_of % 32).astype(jnp.bfloat16)]
    terms += bf16_parts(hweights, 3)
    high = lax.iota(jnp.int32, rows)[:, None] == (slots // lanes)[None, :]
    low = lax.iota(jnp.int32, lanes)[:, None] == (slots % lanes)[None, :]
    left = jnp.concatenate(
        [jnp.where(high, term[None, :], jnp.bfloat16(0)) for term in terms], axis=0
    )
    by_slot = lax.dot_general(
        left,
        low.astype(jnp.bfloat16),
        (((1,), (1,)), ((), ())),
        preferred_element_type=jnp.float32,
    ).reshape(len(terms), total_slots)
    slot_obs = (by_slot[0] * 32 + by_slot[1] + 0.5).astype(jnp.int32)
    slot_hweight = by_slot[2] + by_slot[3] + by_slot[4]

    asked = jnp.stack([table, slot_obs])
    cells_asked = [table[:obs_dev]]
    rows_asked = [slot_obs[:obs_dev]]
    for number, offset in enumerate(halo_moves):
        lower = obs_dev + number * halo_cap
        wanted = passed_along(asked[:, lower : lower + halo_cap], "cell", offset)
        cells_asked.append(wanted[0])
        rows_asked.append(wanted[1] + (number + 1) * obs_dev)
    found = columns(
        jnp.concatenate(cells_asked),
        jnp.concatenate(rows_asked),
        state,
        jnp.concatenate([vertical_weight] + arrived, axis=0),
    )
    pieces = [found[:, :obs_dev]]
    for number, offset in enumerate(halo_moves):
        lower = obs_dev + number * halo_cap
        pieces.append(passed_along(found[:, lower : lower + halo_cap], "cell", -offset))
    equiv = jnp.concatenate(pieces, axis=1) * slot_hweight[None, :]
    mixing = (slot_obs[:, None] == lax.iota(jnp.int32, obs_dev)[None, :]).astype(jnp.bfloat16)
    own_parts = jnp.dot(
        jnp.concatenate(bf16_parts(equiv, 3), axis=0),
        mixing,
        preferred_element_type=jnp.float32,
    )
    own_equiv = own_parts.reshape(3, mem_dev, obs_dev).sum(axis=0)
    sharers = lax.axis_size("mem")
    member = lax.axis_index("mem")
    everyone = jnp.zeros((sharers, mem_dev, obs_dev), jnp.float32)
    everyone = lax.dynamic_update_index_in_dim(everyone, own_equiv, member, 0)
    for by in range(1, sharers):
        everyone = lax.dynamic_update_index_in_dim(
            everyone, passed_along(own_equiv, "mem", by), jnp.mod(member - by, sharers), 0
        )
    everyone = everyone.reshape(sharers * mem_dev, obs_dev)
    mean = jnp.mean(everyone, axis=0, keepdims=True)
    spread_all = everyone - mean
    spread_own = own_equiv - mean
    members = everyone.shape[0]
    inverse = 1.0 / (obs_error * obs_error)
    innov = (obs_value - mean[0]) * inverse
    reg_dev = REG_DEV
    relative = jnp.mod(obs_region - (here - 1) * reg_dev, patches * reg_dev)
    region_ids = lax.iota(jnp.int32, 3 * reg_dev)
    onehot = (region_ids[:, None] == relative[None, :]).astype(jnp.float32)
    masked = (onehot[:, None, :] * spread_own[None, :, :]).reshape(3 * reg_dev * mem_dev, obs_dev)
    scaled_all = spread_all * inverse[None, :]
    cov_part = lax.dot_general(
        masked,
        scaled_all,
        (((1,), (1,)), ((), ())),
        precision=lax.Precision.HIGHEST,
        preferred_element_type=jnp.float32,
    )
    vec_part = jnp.dot(
        masked, innov, precision=lax.Precision.HIGHEST, preferred_element_type=jnp.float32
    )
    sums = jnp.concatenate(
        [cov_part.reshape(3 * reg_dev, mem_dev * members), vec_part.reshape(3 * reg_dev, mem_dev)],
        axis=1,
    )
    from_prev = passed_along(sums[2 * reg_dev :], "cell", 1)
    from_next = passed_along(sums[:reg_dev], "cell", -1)
    summed = sums[reg_dev : 2 * reg_dev] + from_prev + from_next
    cov_matrix = summed[:, : mem_dev * members].reshape(reg_dev, mem_dev, members)
    innovation_proj = summed[:, mem_dev * members :]
    return (cov_matrix, innovation_proj)


def solution(mesh):
    in_specs = (
        P("cell", "mem", None),
        P("cell", None),
        P("cell", None),
        P("cell", None),
        P("cell", None),
        P("cell"),
        P("cell"),
        P("cell"),
    )
    out_specs = (P("cell", "mem", None), P("cell", "mem"))
    return jax.shard_map(
        on_device, mesh=mesh, in_specs=in_specs, out_specs=out_specs, check_vma=False
    )
```
